256 devices in a mesh: fields: 4 (over y, x), rows: 64 (over z, core).
Axes of the slice: x: 2, y: 2, z: 32, core: 2. Of those that a mesh axis runs over, the one named last changes fastest.
The devices are a block of a 4x8x32 slice.
Arguments:
- members: bfloat16 [512, 1048576], P('rows', 'fields'), parts along dimension 1, may hold values from -6 to 6
- predicted: bfloat16 [512, 262144], P('rows', 'fields'), parts along dimension 1, may hold values from -16 to 16
- noise: bfloat16 [512, 262144], P('rows', 'fields'), parts along dimension 1, may hold values from -6 to 6
- observed: float32 [262144], P(('fields', 'rows')), parts along dimension 0, may hold values from -12 to 12
- observation_spread: float32 [262144], P(('fields', 'rows')), parts along dimension 0, may hold values from 1 to 16
Outputs:
- updated: bfloat16 [512, 1048576], P('rows', 'fields'), parts along dimension 1
The draws below stay inside these ranges and needn't reach their ends.
There are 4 independent parts, one for each index of `fields`. The reference program is written for one: setup_inputs(seed, part) draws one part's arguments, and reference() takes and returns one part's arrays. A program takes and returns all parts, laid end to end along the dimension named above; each array names one. Nothing has to cross between parts.
All inputs are finite; a program needn't handle non-finite values.
Results may differ from the reference program's by a relative error of at most 0.005.
Values may be sent and summed in bfloat16 or wider, within the bound.
A program may use at most 64 MiB of HBM per device.

```python
import math
import jax
import jax.numpy as jnp
from jax import lax

NE = 512
NC = 262144
ND = 65536


def with_spikes(values, key, source, target, blocks, factor):
    def block_of(position):
        return (jnp.arange(values.shape[position]) // (values.shape[position] // blocks)).reshape((-1,) + (1,) * (values.ndim - 1 - position))

    near = jax.random.permutation(key, blocks)[block_of(target)]
    far = (block_of(target) + blocks // 2) % blocks
    return jnp.where((block_of(source) == near) | (block_of(source) == far), factor * values, values)


def shard_levels(own_key, shape, split, least, largest):
    def one(dim, blocks):
        steps = jax.random.uniform(jax.random.fold_in(jax.random.fold_in(own_key, 6), dim), (blocks,), jnp.float32, least / len(split), largest / len(split))
        return jnp.repeat(jnp.exp(steps), shape[dim] // blocks).reshape((-1,) + (1,) * (len(shape) - dim - 1))

    level = one(*split[0])
    for cut in split[1:]:
        level = level * one(*cut)
    return level


def bell_draw(key, shape, deviation, limit, split=(), held_as=jnp.bfloat16):
    array = deviation * jax.random.normal(key, shape, jnp.float32)
    if split:
        array = array * shard_levels(key, shape, split, -0.22, 0.18)
    return jnp.clip(array, -limit, limit).astype(held_as)


def gaussian_with(stream_key, shape, deviation, limit, shards, heavy, kind=jnp.bfloat16):
    result = deviation * jax.random.normal(stream_key, shape, jnp.float32)
    if shards:
        result = result * shard_levels(stream_key, shape, shards, -0.22, 0.18)
    return jnp.clip(with_spikes(result, jax.random.fold_in(stream_key, 3), *heavy), -limit, limit).astype(kind)


def setup_inputs(seed: int = 0, part: int = 0) -> dict:
    seeds = jax.random.split(jax.random.key(seed), 6)
    own_keys = jax.random.split(jax.random.fold_in(seeds[5], part), 6)
    return {
        "members": bell_draw(own_keys[0], (NE, NC), 1.0, 6.0, ((0, 64),)),
        "predicted": gaussian_with(own_keys[1], (NE, ND), 1.0, 16.0, ((0, 64),), (1, 0, 64, 4.0)),
        "noise": bell_draw(own_keys[2], (NE, ND), 1.0, 6.0, ((0, 64),)),
        "observed": bell_draw(own_keys[3], (ND,), 2.0, 12.0, ((0, 64),), jnp.float32),
        "observation_spread": jnp.clip(jnp.exp(math.log(16.0) - 2.7725887 * jax.random.uniform(own_keys[4], (ND,), jnp.float32) ** shard_levels(own_keys[4], (ND,), ((0, 64),), -0.2, 0.2)), 1.0, 16.0),
    }


damping = 21.0

def reference(members, predicted, noise, observed, observation_spread):
    inverse_square_root = 1.0 / math.sqrt(NE - 1)
    predicted_response = predicted.astype(jnp.float32)
    ensemble_data_average = lax.optimization_barrier(jnp.mean(predicted_response, axis=0))
    standardized_anomalies = ((predicted_response - ensemble_data_average) * (inverse_square_root / observation_spread)).astype(jnp.bfloat16)
    measurement_residual = ((observed - predicted_response) / observation_spread + noise.astype(jnp.float32)).astype(jnp.bfloat16)
    gram_matrix = lax.dot_general(standardized_anomalies.astype(jnp.float32), standardized_anomalies.astype(jnp.float32), (((1,), (1,)), ((), ())), preferred_element_type=jnp.float32)
    cross_terms = lax.dot_general(standardized_anomalies.astype(jnp.float32), measurement_residual.astype(jnp.float32), (((1,), (1,)), ((), ())), preferred_element_type=jnp.float32)
    system = gram_matrix + damping * jnp.eye(NE, dtype=jnp.float32)
    factor = jnp.linalg.cholesky(system)
    weights = jax.scipy.linalg.cho_solve((factor, True), cross_terms).astype(jnp.bfloat16)
    params = members.astype(jnp.float32)
    cell_mean = lax.optimization_barrier(jnp.mean(params, axis=0))
    anomaly = ((params - cell_mean) * inverse_square_root).astype(jnp.bfloat16)
    update = lax.dot_general(weights.astype(jnp.float32), anomaly.astype(jnp.float32), (((0,), (0,)), ((), ())), preferred_element_type=jnp.float32)
    return (params + update).astype(jnp.bfloat16)
```

```python
import functools
import math

import jax
import jax.numpy as jnp
from jax import lax
from jax.experimental import pallas as pl
from jax.experimental.pallas import tpu as pltpu
from jax.sharding import PartitionSpec as P

ROWS = "rows"
MESH = pl.DeviceIdType.MESH
DAMPING = 21.0
CHUNKS = 4
BLOCK = 128
F32 = jnp.float32
BF16 = jnp.bfloat16


def drain(ref, sem):
    pltpu.make_async_copy(ref, ref, sem).wait()


def exact_dot(a, b):
    return jnp.dot(a, b, precision=lax.Precision.HIGHEST, preferred_element_type=F32)


def inverse_in_place(block):
    size = block.shape[0]
    lane = lax.broadcasted_iota(jnp.int32, (size, size), 1)
    line = lax.broadcasted_iota(jnp.int32, (size, size), 0)
    lane_row = lax.broadcasted_iota(jnp.int32, (1, size), 1)

    def step(p, carry):
        held = block[...]
        row = block[pl.ds(p, 1), :]
        pivot = 1.0 / jnp.sum(jnp.where(lane_row == p, row, 0.0), axis=1, keepdims=True)
        column = jnp.sum(jnp.where(lane == p, held, 0.0), axis=1, keepdims=True)
        scaled = jnp.where(lane_row == p, pivot, row * pivot)
        column = jnp.where(line[:, :1] == p, -1.0, column)
        kept = jnp.where((lane == p) | (line == p), 0.0, held)
        block[...] = kept - column * scaled
        return carry

    lax.fori_loop(0, size, step, 0)


def kernel(
    n, members, predicted, noise, observed, spread, out,
    pred_in, noise_in, cells_in, cells_out, white, innov, part, part_in,
    sum_right, sum_left, in_right, in_left, total, table, pivots, weights, anomaly,
    own_sem, data_send, data_sem, in_send, in_sem, out_send, out_sem, pair_send, pair_sem,
    rs_send, rs_right, rs_left, ag_send, ag_right, ag_left, weight_send, weight_sem, own_out,
):
    nz = n // 2
    half = nz // 2
    me = lax.axis_index(ROWS)
    z, core = lax.div(me, 2), lax.rem(me, 2)
    local, cells = members.shape[0], members.shape[1] // n
    data = predicted.shape[1] // n
    count = n * local
    width = cells // CHUNKS
    scale = 1.0 / math.sqrt(count - 1)

    def remote(src, dst, send_sem, recv_sem, peer):
        pltpu.make_async_remote_copy(
            src_ref=src, dst_ref=dst, send_sem=send_sem, recv_sem=recv_sem,
            device_id={ROWS: peer}, device_id_type=MESH,
        ).start()

    def to_peers(send):
        def at(shift, other):
            send(lax.rem(z + shift, nz) * 2 + lax.rem(core + other, 2))

        at(half, 0)
        at(half, 1)

        def both_ways(i, carry):
            for other in (0, 1):
                at(half - i, other)
                at(half + i, other)
            return carry

        lax.fori_loop(1, half, both_ways, 0)
        at(0, 1)

    def span(index, size, offset=0):
        return pl.ds(pl.multiple_of(index * size + offset, 128), size)

    barrier = pltpu.get_barrier_semaphore()

    def greet(i, carry):
        pl.semaphore_signal(barrier, inc=1, device_id={ROWS: lax.rem(me + i, n)}, device_id_type=MESH)
        return carry

    lax.fori_loop(1, n, greet, 0)
    own_pred = pltpu.make_async_copy(predicted.at[:, span(me, data)], pred_in.at[me], own_sem.at[0])
    own_noise = pltpu.make_async_copy(noise.at[:, span(me, data)], noise_in.at[me], own_sem.at[1])
    own_cells = pltpu.make_async_copy(members.at[:, span(me, cells)], cells_in.at[me], own_sem.at[2])
    own_pred.start()
    own_noise.start()
    own_cells.start()
    pl.semaphore_wait(barrier, n - 1)

    def send_data(peer):
        remote(predicted.at[:, span(peer, data)], pred_in.at[me], data_send.at[0], data_sem.at[0], peer)
        remote(noise.at[:, span(peer, data)], noise_in.at[me], data_send.at[1], data_sem.at[1], peer)

    def send_cells(k):
        def send(peer):
            remote(
                members.at[:, pl.ds(pl.multiple_of(peer * cells + k * width, 128), width)],
                cells_in.at[me, :, pl.ds(pl.multiple_of(k * width, 128), width)],
                in_send, in_sem.at[k], peer,
            )

        to_peers(send)

    to_peers(send_data)

    @pl.when(core == 0)
    def _():
        send_cells(0)

    own_pred.wait()
    own_noise.wait()
    drain(pred_in.at[pl.ds(0, n - 1)], data_sem.at[0])
    drain(noise_in.at[pl.ds(0, n - 1)], data_sem.at[1])

    def add_rows(i, acc):
        return acc + pred_in[i].astype(F32)

    sums = lax.fori_loop(0, n, add_rows, jnp.zeros((local, data), F32))
    mean = jnp.sum(sums, axis=0, keepdims=True) * (1.0 / count)
    spreads = spread[...]
    factor = scale / spreads
    target = observed[...]

    def standardize(i, carry):
        x = pred_in[pl.ds(2 * i, 2)].astype(F32).reshape(2 * local, data)
        e = noise_in[pl.ds(2 * i, 2)].astype(F32).reshape(2 * local, data)
        rows = pl.ds(pl.multiple_of(2 * local * i, 2 * local), 2 * local)
        white[rows, :] = ((x - mean) * factor).astype(BF16)
        innov[rows, :] = ((target - x) / spreads + e).astype(BF16)
        return carry

    lax.fori_loop(0, n // 2, standardize, 0)
    lines = part.shape[1]
    along = (((1,), (1,)), ((), ()))

    def products(i, carry):
        rows = white[pl.ds(pl.multiple_of(BLOCK * i, BLOCK), BLOCK), :]
        gram = lax.dot_general(rows, white[...], along, preferred_element_type=F32)
        cross = lax.dot_general(rows, innov[...], along, preferred_element_type=F32)
        slabs = pl.ds(i * (BLOCK // lines), BLOCK // lines)
        part[slabs, :, :count] = gram.reshape(BLOCK // lines, lines, count)
        part[slabs, :, count:] = cross.reshape(BLOCK // lines, lines, count)
        return carry

    lax.fori_loop(0, count // BLOCK, products, 0)

    @pl.when(core == 0)
    def _():
        remote(part, part_in, pair_send, pair_sem, me + 1)

        def rest(k, carry):
            send_cells(k)
            return carry

        lax.fori_loop(1, CHUNKS, rest, 0)
        drain(part, pair_send)
        drain(weights, weight_sem)

    @pl.when(core == 1)
    def _():
        drain(part_in, pair_sem)
        right = lax.rem(z + 1, nz) * 2 + 1
        left = lax.rem(z + nz - 1, nz) * 2 + 1

        def pair(j):
            return part[j] + part_in[j]

        def reduce_right(i, first=False):
            j = lax.rem(z + half + nz - i, nz)
            value = pair(j)
            if not first:
                drain(in_right.at[i - 1], rs_right.at[i - 1])
                value = value + in_right[i - 1]
            sum_right[i] = value
            remote(sum_right.at[i], in_right.at[i], rs_send.at[0], rs_right.at[i], right)

        def reduce_left(i, first=False):
            j = lax.rem(z + nz - half + 1 + i, nz)
            value = pair(j)
            if not first:
                drain(in_left.at[i - 1], rs_left.at[i - 1])
                value = value + in_left[i - 1]
            sum_left[i] = value
            remote(sum_left.at[i], in_left.at[i], rs_send.at[1], rs_left.at[i], left)

        reduce_right(0, True)
        reduce_left(0, True)

        def reduce(i, carry):
            reduce_right(i)
            reduce_left(i)
            return carry

        lax.fori_loop(1, half - 1, reduce, 0)
        reduce_right(half - 1)
        drain(in_left.at[half - 2], rs_left.at[half - 2])
        drain(in_right.at[half - 1], rs_right.at[half - 1])
        total[z] = pair(z) + in_left[half - 2] + in_right[half - 1]

        def spread_right(i, first=False):
            j = lax.rem(z + nz - i, nz)
            if not first:
                drain(total.at[j], ag_right.at[i - 1])
            remote(total.at[j], total.at[j], ag_send.at[0], ag_right.at[i], right)

        def spread_left(i, first=False):
            j = lax.rem(z + i, nz)
            if not first:
                drain(total.at[j], ag_left.at[i - 1])
            remote(total.at[j], total.at[j], ag_send.at[1], ag_left.at[i], left)

        spread_right(0, True)
        spread_left(0, True)

        def spread_on(i, carry):
            spread_right(i)
            spread_left(i)
            return carry

        lax.fori_loop(1, half - 1, spread_on, 0)
        spread_right(half - 1)
        drain(total.at[0], ag_left.at[half - 2])
        drain(total.at[0], ag_right.at[half - 1])

        def all_cells(k, carry):
            send_cells(k)
            return carry

        lax.fori_loop(0, CHUNKS, all_cells, 0)

        def unpack(j, carry):
            table[pl.ds(pl.multiple_of(j * lines, lines), lines), :] = total[j]
            return carry

        lax.fori_loop(0, nz, unpack, 0)
        blocks = count // BLOCK
        eye = lax.broadcasted_iota(jnp.int32, (BLOCK, BLOCK), 0) == lax.broadcasted_iota(
            jnp.int32, (BLOCK, BLOCK), 1
        )
        for k in range(blocks):
            here = slice(k * BLOCK, (k + 1) * BLOCK)
            ahead = slice((k + 1) * BLOCK, 2 * count)
            pivots[...] = table[here, here] + jnp.where(eye, DAMPING, 0.0)
            inverse_in_place(pivots)
            table[here, ahead] = exact_dot(pivots[...], table[here, ahead])
            for i in range(k + 1, blocks):
                rows = slice(i * BLOCK, (i + 1) * BLOCK)
                table[rows, ahead] = table[rows, ahead] - exact_dot(table[rows, here], table[here, ahead])
        for k in reversed(range(blocks)):
            here = slice(k * BLOCK, (k + 1) * BLOCK)
            if k < blocks - 1:
                table[here, count:] = table[here, count:] - exact_dot(
                    table[here, (k + 1) * BLOCK : count], table[(k + 1) * BLOCK : count, count:]
                )
        for k in range(blocks):
            here = slice(k * BLOCK, (k + 1) * BLOCK)
            weights[:, here] = table[here, count:].T.astype(BF16)
        remote(weights, weights, weight_send, weight_sem, me - 1)
        drain(weights, weight_send)
        drain(total.at[pl.ds(0, half)], rs_send.at[0])
        drain(total.at[pl.ds(0, half - 1)], rs_send.at[1])
        drain(total.at[pl.ds(0, half)], ag_send.at[0])
        drain(total.at[pl.ds(0, half - 1)], ag_send.at[1])

    own_cells.wait()

    def update(k, carry):
        columns = pl.ds(pl.multiple_of(k * width, 128), width)
        drain(cells_in.at[pl.ds(0, n - 1), :, columns], in_sem.at[k])

        def add_cells(i, acc):
            return acc + cells_in[i, :, columns].astype(F32)

        sums = lax.fori_loop(0, n, add_cells, jnp.zeros((local, width), F32))
        mean = jnp.sum(sums, axis=0, keepdims=True) * (1.0 / count)

        def center(i, inner):
            x = cells_in[pl.ds(2 * i, 2), :, columns].astype(F32).reshape(2 * local, width)
            rows = pl.ds(pl.multiple_of(2 * local * i, 2 * local), 2 * local)
            anomaly[rows, :] = ((x - mean) * scale).astype(BF16)
            return inner

        lax.fori_loop(0, n // 2, center, 0)

        def renew(i, inner):
            rows = pl.ds(pl.multiple_of(BLOCK * i, BLOCK), BLOCK)
            slabs = pl.ds(i * (BLOCK // local), BLOCK // local)
            change = jnp.dot(weights[rows, :], anomaly[...], preferred_element_type=F32)
            x = cells_in[slabs, :, columns].astype(F32)
            cells_out[slabs, :, columns] = (x + change.reshape(x.shape)).astype(BF16)
            return inner

        lax.fori_loop(0, count // BLOCK, renew, 0)

        def send(peer):
            remote(
                cells_out.at[peer, :, columns],
                out.at[:, pl.ds(pl.multiple_of(me * cells + k * width, 128), width)],
                out_send, out_sem, peer,
            )

        to_peers(send)
        return carry

    lax.fori_loop(0, CHUNKS, update, 0)
    mine = pltpu.make_async_copy(cells_out.at[me], out.at[:, span(me, cells)], own_out)
    mine.start()
    drain(pred_in.at[pl.ds(0, n - 1)], data_send.at[0])
    drain(noise_in.at[pl.ds(0, n - 1)], data_send.at[1])
    drain(cells_in.at[pl.ds(0, n - 1)], in_send)
    drain(cells_out.at[pl.ds(0, n - 1)], out_send)
    drain(cells_out.at[pl.ds(0, n - 1)], out_sem)
    mine.wait()


def solution(mesh):
    n = mesh.shape[ROWS]

    def on_device(members, predicted, noise, observed, spread):
        local = members.shape[0]
        count, nz = n * local, n // 2
        cells, data = members.shape[1] // n, predicted.shape[1] // n
        half, lines = nz // 2, count // nz
        slab = (lines, 2 * count)
        anywhere = pl.BlockSpec(memory_space=pltpu.HBM)
        on_chip = pl.BlockSpec(memory_space=pltpu.VMEM)
        dma = pltpu.SemaphoreType.DMA
        return pl.pallas_call(
            functools.partial(kernel, n),
            name="smoother",
            out_shape=jax.ShapeDtypeStruct(members.shape, members.dtype),
            in_specs=[anywhere, anywhere, anywhere, on_chip, on_chip],
            out_specs=anywhere,
            scratch_shapes=[
                pltpu.VMEM((n, local, data), BF16),
                pltpu.VMEM((n, local, data), BF16),
                pltpu.VMEM((n, local, cells), BF16),
                pltpu.VMEM((n, local, cells), BF16),
                pltpu.VMEM((count, data), BF16),
                pltpu.VMEM((count, data), BF16),
                pltpu.VMEM((nz, *slab), F32),
                pltpu.VMEM((nz, *slab), F32),
                pltpu.VMEM((half, *slab), F32),
                pltpu.VMEM((half, *slab), F32),
                pltpu.VMEM((half, *slab), F32),
                pltpu.VMEM((half, *slab), F32),
                pltpu.VMEM((nz, *slab), F32),
                pltpu.VMEM((count, 2 * count), F32),
                pltpu.VMEM((BLOCK, BLOCK), F32),
                pltpu.VMEM((count, count), BF16),
                pltpu.VMEM((count, cells // CHUNKS), BF16),
                dma((3,)), dma((2,)), dma((2,)), dma, dma((CHUNKS,)), dma, dma, dma, dma,
                dma((2,)), dma((half,)), dma((half,)), dma((2,)), dma((half,)), dma((half,)),
                dma, dma, dma,
            ],
            compiler_params=pltpu.CompilerParams(collective_id=0, has_side_effects=True),
        )(members, predicted, noise, observed.reshape(1, data), spread.reshape(1, data))

    placed = (P(ROWS, "fields"), P(ROWS, "fields"), P(ROWS, "fields"), P(("fields", ROWS)), P(("fields", ROWS)))
    return jax.shard_map(
        on_device, mesh=mesh, in_specs=placed, out_specs=P(ROWS, "fields"), check_vma=False
    )
```

```python
import functools
import math

import jax
import jax.numpy as jnp
from jax import lax
from jax.experimental import pallas as pl
from jax.experimental.pallas import tpu as pltpu
from jax.sharding import PartitionSpec as P

ROWS = "rows"
MESH = pl.DeviceIdType.MESH
DAMPING = 21.0
CHUNKS = 4
RELAYED = 3
BLOCK = 128
F32 = jnp.float32
BF16 = jnp.bfloat16


def drain(ref, sem):
    pltpu.make_async_copy(ref, ref, sem).wait()


def exact_dot(a, b):
    return jnp.dot(a, b, precision=lax.Precision.HIGHEST, preferred_element_type=F32)


def halves_of(lines):
    first = (lines // 8 + 1) // 2 * 8
    return ((0, first), (first, lines - first))


def inverse_in_place(block):
    size = block.shape[0]
    lane = lax.broadcasted_iota(jnp.int32, (size, size), 1)
    line = lax.broadcasted_iota(jnp.int32, (size, size), 0)
    lane_row = lax.broadcasted_iota(jnp.int32, (1, size), 1)

    def step(p, carry):
        held = block[...]
        row = block[pl.ds(p, 1), :]
        pivot = 1.0 / jnp.sum(jnp.where(lane_row == p, row, 0.0), axis=1, keepdims=True)
        column = jnp.sum(jnp.where(lane == p, held, 0.0), axis=1, keepdims=True)
        scaled = jnp.where(lane_row == p, pivot, row * pivot)
        column = jnp.where(line[:, :1] == p, -1.0, column)
        kept = jnp.where((lane == p) | (line == p), 0.0, held)
        block[...] = kept - column * scaled
        return carry

    lax.fori_loop(0, size, step, 0)


def kernel(
    n, members, predicted, noise, observed, spread, out,
    pred_in, noise_in, cells_in, cells_out, relay, white, innov, part, part_in,
    sum_right, sum_left, in_right, in_left, total, table, pivots, weights, anomaly,
    own_sem, data_send, data_sem, in_send, in_sem, out_send, out_sem, pair_send, pair_sem,
    rs_send, rs_right, rs_left, ag_send, ag_right, ag_left, weight_send, weight_sem,
    relay_send, relay_sem, beside_send, relayed_send, own_out,
):
    nz = n // 2
    half = nz // 2
    me = lax.axis_index(ROWS)
    z, core = lax.div(me, 2), lax.rem(me, 2)
    local, cells = members.shape[0], members.shape[1] // n
    data = predicted.shape[1] // n
    count = n * local
    width = cells // CHUNKS
    scale = 1.0 / math.sqrt(count - 1)
    blocks = count // BLOCK
    lines = part.shape[0] // nz

    def remote(src, dst, send_sem, recv_sem, peer):
        pltpu.make_async_remote_copy(
            src_ref=src, dst_ref=dst, send_sem=send_sem, recv_sem=recv_sem,
            device_id={ROWS: peer}, device_id_type=MESH,
        ).start()

    def to_other_chips(send):
        def at(shift):
            for other in (0, 1):
                send(lax.rem(z + shift, nz) * 2 + lax.rem(core + other, 2))

        at(half)

        def both_ways(i, carry):
            at(half - i)
            at(half + i)
            return carry

        lax.fori_loop(1, half, both_ways, 0)

    def to_peers(send):
        to_other_chips(send)
        send(z * 2 + 1 - core)

    def span(index, size):
        return pl.ds(pl.multiple_of(index * size, 128), size)

    def piece(index, k):
        return pl.ds(pl.multiple_of(index * cells + k * width, 128), width)
    barrier = pltpu.get_barrier_semaphore()

    def greet(i, carry):
        pl.semaphore_signal(barrier, inc=1, device_id={ROWS: lax.rem(me + i, n)}, device_id_type=MESH)
        return carry

    lax.fori_loop(1, n, greet, 0)
    own_pred = pltpu.make_async_copy(predicted.at[:, span(me, data)], pred_in.at[me], own_sem.at[0])
    own_noise = pltpu.make_async_copy(noise.at[:, span(me, data)], noise_in.at[me], own_sem.at[1])
    own_cells = pltpu.make_async_copy(members.at[:, span(me, cells)], cells_in.at[me], own_sem.at[2])
    own_pred.start()
    own_noise.start()
    own_cells.start()
    pl.semaphore_wait(barrier, n - 1)

    def send_data(peer):
        remote(predicted.at[:, span(peer, data)], pred_in.at[me], data_send.at[0], data_sem.at[0], peer)
        remote(noise.at[:, span(peer, data)], noise_in.at[me], data_send.at[1], data_sem.at[1], peer)

    def send_cells(k):
        def send(peer):
            remote(members.at[:, piece(peer, k)], cells_in.at[me, :, piece(0, k)], in_send, in_sem.at[k], peer)

        to_peers(send)

    def pass_cells(k):
        def send(peer):
            remote(relay.at[:, piece(peer, k)], cells_in.at[me + 1, :, piece(0, k)], relayed_send, in_sem.at[k], peer)

        to_other_chips(send)
    to_peers(send_data)

    @pl.when(core == 0)
    def _():
        send_cells(0)

    @pl.when(core == 1)
    def _():
        remote(members, relay, relay_send, relay_sem, me - 1)

        def beside(k, carry):
            remote(
                members.at[:, piece(me - 1, k)], cells_in.at[me, :, piece(0, k)], beside_send, in_sem.at[k], me - 1
            )
            return carry

        lax.fori_loop(0, RELAYED, beside, 0)
    own_pred.wait()
    own_noise.wait()
    drain(pred_in.at[pl.ds(0, n - 1)], data_sem.at[0])
    drain(noise_in.at[pl.ds(0, n - 1)], data_sem.at[1])

    def add_rows(i, acc):
        return acc + pred_in[i].astype(F32)

    sums = lax.fori_loop(0, n, add_rows, jnp.zeros((local, data), F32))
    mean = jnp.sum(sums, axis=0, keepdims=True) * (1.0 / count)
    spreads = spread[...]
    factor = scale / spreads
    target = observed[...]

    def standardize(i, carry):
        x = pred_in[pl.ds(2 * i, 2)].astype(F32).reshape(2 * local, data)
        e = noise_in[pl.ds(2 * i, 2)].astype(F32).reshape(2 * local, data)
        rows = pl.ds(pl.multiple_of(2 * local * i, 2 * local), 2 * local)
        white[rows, :] = ((x - mean) * factor).astype(BF16)
        innov[rows, :] = ((target - x) / spreads + e).astype(BF16)
        return carry

    lax.fori_loop(0, n // 2, standardize, 0)
    along = (((1,), (1,)), ((), ()))
    panels = []
    for i in range(blocks):
        start = sum(2 * blocks - k for k in range(i)) * BLOCK
        panels.append(start)
        rows = white[i * BLOCK : (i + 1) * BLOCK, :]
        gram = lax.dot_general(rows, white[i * BLOCK :, :], along, preferred_element_type=F32)
        cross = lax.dot_general(rows, innov[...], along, preferred_element_type=F32)
        for k in range(blocks - i):
            part[start + k * BLOCK : start + (k + 1) * BLOCK, :] = gram[:, k * BLOCK : (k + 1) * BLOCK]
        start += (blocks - i) * BLOCK
        for k in range(blocks):
            part[start + k * BLOCK : start + (k + 1) * BLOCK, :] = cross[:, k * BLOCK : (k + 1) * BLOCK]

    @pl.when(core == 0)
    def _():
        remote(part, part_in, pair_send, pair_sem, me + 1)
        drain(relay, relay_sem)

        def rest(k, carry):
            pass_cells(k)
            send_cells(k + 1)
            return carry

        lax.fori_loop(0, min(RELAYED, CHUNKS - 1), rest, 0)
        if RELAYED == CHUNKS:
            pass_cells(CHUNKS - 1)
        drain(part, pair_send)
        drain(weights, weight_sem)

    @pl.when(core == 1)
    def _():
        drain(part_in, pair_sem)
        right = lax.rem(z + 1, nz) * 2 + 1
        left = lax.rem(z + nz - 1, nz) * 2 + 1
        halves = halves_of(lines)

        def slab(j, start, size):
            return pl.ds(pl.multiple_of(j * lines + start, 8), size)

        def pair(j, h):
            return part[slab(j, *halves[h]), :] + part_in[slab(j, *halves[h]), :]

        def reduce_one(i, j, h, first, sums, landed, side, sems, peer):
            rows = pl.ds(*halves[h])
            value = pair(j, h)
            if not first:
                drain(landed.at[i - 1, rows], sems.at[h, i - 1])
                value = value + landed[i - 1, rows]
            sums[i, rows] = value
            remote(sums.at[i, rows], landed.at[i, rows], rs_send.at[side], sems.at[h, i], peer)

        def reduce_right(i, h, first=False):
            reduce_one(i, lax.rem(z + half + nz - i, nz), h, first, sum_right, in_right, 0, rs_right, right)

        def reduce_left(i, h, first=False):
            reduce_one(i, lax.rem(z + nz - half + 1 + i, nz), h, first, sum_left, in_left, 1, rs_left, left)

        for h in (0, 1):
            reduce_right(0, h, True)
            reduce_left(0, h, True)

        def reduce(i, carry):
            for h in (0, 1):
                reduce_right(i, h)
                reduce_left(i, h)
            return carry

        lax.fori_loop(1, half - 1, reduce, 0)
        for h in (0, 1):
            reduce_right(half - 1, h)
        for h in (0, 1):
            rows = pl.ds(*halves[h])
            drain(in_left.at[half - 2, rows], rs_left.at[h, half - 2])
            drain(in_right.at[half - 1, rows], rs_right.at[h, half - 1])
            total[slab(z, *halves[h]), :] = pair(z, h) + in_left[half - 2, rows] + in_right[half - 1, rows]

        def spread_one(i, j, h, first, side, sems, peer):
            rows = slab(j, *halves[h])
            if not first:
                drain(total.at[rows], sems.at[h, i - 1])
            remote(total.at[rows], total.at[rows], ag_send.at[side], sems.at[h, i], peer)

        def spread_right(i, h, first=False):
            spread_one(i, lax.rem(z + nz - i, nz), h, first, 0, ag_right, right)

        def spread_left(i, h, first=False):
            spread_one(i, lax.rem(z + i, nz), h, first, 1, ag_left, left)

        for h in (0, 1):
            spread_right(0, h, True)
            spread_left(0, h, True)

        def spread_on(i, carry):
            for h in (0, 1):
                spread_right(i, h)
                spread_left(i, h)
            return carry

        lax.fori_loop(1, half - 1, spread_on, 0)
        for h in (0, 1):
            spread_right(half - 1, h)
        for h in (0, 1):
            drain(total.at[pl.ds(0, halves[h][1])], ag_left.at[h, half - 2])
            drain(total.at[pl.ds(0, halves[h][1])], ag_right.at[h, half - 1])

        def rest(k, carry):
            send_cells(k)
            return carry

        lax.fori_loop(RELAYED, CHUNKS, rest, 0)
        for i in range(blocks):
            for k in range(2 * blocks - i):
                table[i * BLOCK : (i + 1) * BLOCK, (i + k) * BLOCK : (i + k + 1) * BLOCK] = total[
                    panels[i] + k * BLOCK : panels[i] + (k + 1) * BLOCK, :
                ]
        eye = lax.broadcasted_iota(jnp.int32, (BLOCK, BLOCK), 0) == lax.broadcasted_iota(
            jnp.int32, (BLOCK, BLOCK), 1
        )
        for k in range(blocks):
            here = slice(k * BLOCK, (k + 1) * BLOCK)
            ahead = slice((k + 1) * BLOCK, 2 * count)
            pivots[...] = table[here, here] + jnp.where(eye, DAMPING, 0.0)
            inverse_in_place(pivots)
            panel = table[here, ahead]
            scaled = exact_dot(pivots[...], panel)
            for i in range(k + 1, blocks):
                start = (i - k - 1) * BLOCK
                across = panel[:, start : start + BLOCK].T
                rows = slice(i * BLOCK, (i + 1) * BLOCK)
                table[rows, i * BLOCK :] = table[rows, i * BLOCK :] - exact_dot(across, scaled[:, start:])
            table[here, ahead] = scaled
        for k in reversed(range(blocks - 1)):
            here = slice(k * BLOCK, (k + 1) * BLOCK)
            table[here, count:] = table[here, count:] - exact_dot(
                table[here, (k + 1) * BLOCK : count], table[(k + 1) * BLOCK : count, count:]
            )
        for k in range(blocks):
            here = slice(k * BLOCK, (k + 1) * BLOCK)
            weights[:, here] = table[here, count:].T.astype(BF16)
        remote(weights, weights, weight_send, weight_sem, me - 1)

    own_cells.wait()

    def update(k, carry):
        columns = piece(0, k)
        drain(cells_in.at[pl.ds(0, n - 1), :, columns], in_sem.at[k])

        def add_cells(i, acc):
            return acc + cells_in[i, :, columns].astype(F32)

        sums = lax.fori_loop(0, n, add_cells, jnp.zeros((local, width), F32))
        mean = jnp.sum(sums, axis=0, keepdims=True) * (1.0 / count)

        def center(i, inner):
            x = cells_in[pl.ds(2 * i, 2), :, columns].astype(F32).reshape(2 * local, width)
            rows = pl.ds(pl.multiple_of(2 * local * i, 2 * local), 2 * local)
            anomaly[rows, :] = ((x - mean) * scale).astype(BF16)
            return inner

        lax.fori_loop(0, n // 2, center, 0)

        def renew(i, inner):
            rows = pl.ds(pl.multiple_of(BLOCK * i, BLOCK), BLOCK)
            slabs = pl.ds(i * (BLOCK // local), BLOCK // local)
            change = jnp.dot(weights[rows, :], anomaly[...], preferred_element_type=F32)
            x = cells_in[slabs, :, columns].astype(F32)
            cells_out[slabs, :, columns] = (x + change.reshape(x.shape)).astype(BF16)
            return inner

        lax.fori_loop(0, blocks, renew, 0)

        def send(peer):
            remote(cells_out.at[peer, :, columns], out.at[:, piece(me, k)], out_send, out_sem, peer)

        to_peers(send)
        return carry

    lax.fori_loop(0, CHUNKS, update, 0)
    mine = pltpu.make_async_copy(cells_out.at[me], out.at[:, span(me, cells)], own_out)
    mine.start()
    drain(pred_in.at[pl.ds(0, n - 1)], data_send.at[0])
    drain(noise_in.at[pl.ds(0, n - 1)], data_send.at[1])

    @pl.when(core == 0)
    def _():
        drain(cells_in.at[pl.ds(0, n - 1)], in_send)
        drain(cells_in.at[pl.ds(0, n - 2), :, pl.ds(0, RELAYED * width)], relayed_send)

    @pl.when(core == 1)
    def _():
        if RELAYED < CHUNKS:
            drain(cells_in.at[pl.ds(0, n - 1), :, pl.ds(0, (CHUNKS - RELAYED) * width)], in_send)
        drain(members, relay_send)
        drain(cells_in.at[0, :, pl.ds(0, RELAYED * width)], beside_send)
        drain(weights, weight_send)
        drain(total.at[pl.ds(0, half * lines)], rs_send.at[0])
        drain(total.at[pl.ds(0, (half - 1) * lines)], rs_send.at[1])
        drain(total.at[pl.ds(0, half * lines)], ag_send.at[0])
        drain(total.at[pl.ds(0, (half - 1) * lines)], ag_send.at[1])

    drain(cells_out.at[pl.ds(0, n - 1)], out_send)
    drain(cells_out.at[pl.ds(0, n - 1)], out_sem)
    mine.wait()


def solution(mesh):
    n = mesh.shape[ROWS]

    def on_device(members, predicted, noise, observed, spread):
        local = members.shape[0]
        count, nz = n * local, n // 2
        cells, data = members.shape[1] // n, predicted.shape[1] // n
        half, blocks = nz // 2, count // BLOCK
        packed = (blocks * (blocks + 1) // 2 + blocks * blocks) * BLOCK
        lines = packed // nz
        anywhere = pl.BlockSpec(memory_space=pltpu.HBM)
        on_chip = pl.BlockSpec(memory_space=pltpu.VMEM)
        dma = pltpu.SemaphoreType.DMA
        return pl.pallas_call(
            functools.partial(kernel, n),
            name="smoother",
            out_shape=jax.ShapeDtypeStruct(members.shape, members.dtype),
            in_specs=[anywhere, anywhere, anywhere, on_chip, on_chip],
            out_specs=anywhere,
            scratch_shapes=[
                pltpu.VMEM((n, local, data), BF16),
                pltpu.VMEM((n, local, data), BF16),
                pltpu.VMEM((n, local, cells), BF16),
                pltpu.VMEM((n, local, cells), BF16),
                pltpu.VMEM(members.shape, BF16),
                pltpu.VMEM((count, data), BF16),
                pltpu.VMEM((count, data), BF16),
                pltpu.VMEM((packed, BLOCK), F32),
                pltpu.VMEM((packed, BLOCK), F32),
                pltpu.VMEM((half, lines, BLOCK), F32),
                pltpu.VMEM((half, lines, BLOCK), F32),
                pltpu.VMEM((half, lines, BLOCK), F32),
                pltpu.VMEM((half, lines, BLOCK), F32),
                pltpu.VMEM((packed, BLOCK), F32),
                pltpu.VMEM((count, 2 * count), F32),
                pltpu.VMEM((BLOCK, BLOCK), F32),
                pltpu.VMEM((count, count), BF16),
                pltpu.VMEM((count, cells // CHUNKS), BF16),
                dma((3,)), dma((2,)), dma((2,)), dma, dma((CHUNKS,)), dma, dma, dma, dma,
                dma((2,)), dma((2, half)), dma((2, half)), dma((2,)), dma((2, half)), dma((2, half)),
                dma, dma, dma, dma, dma, dma, dma,
            ],
            compiler_params=pltpu.CompilerParams(collective_id=0, has_side_effects=True),
        )(members, predicted, noise, observed.reshape(1, data), spread.reshape(1, data))

    placed = (P(ROWS, "fields"), P(ROWS, "fields"), P(ROWS, "fields"), P(("fields", ROWS)), P(("fields", ROWS)))
    return jax.shard_map(
        on_device, mesh=mesh, in_specs=placed, out_specs=P(ROWS, "fields"), check_vma=False
    )
```

```python
import functools
import math

import jax
import jax.numpy as jnp
from jax import lax
from jax.experimental import pallas as pl
from jax.experimental.pallas import tpu as pltpu
from jax.sharding import PartitionSpec as P

ROWS = "rows"
MESH = pl.DeviceIdType.MESH
DAMPING = 21.0
CHUNKS = 4
RELAYED = 3
NEAR = 4
BLOCK = 128
F32 = jnp.float32
BF16 = jnp.bfloat16


def drain(ref, sem):
    pltpu.make_async_copy(ref, ref, sem).wait()


def exact_dot(a, b):
    return jnp.dot(a, b, precision=lax.Precision.HIGHEST, preferred_element_type=F32)


def halves_of(lines):
    first = (lines // 8 + 1) // 2 * 8
    return ((0, first), (first, lines - first))


def inverse_in_place(block):
    size = block.shape[0]
    lane = lax.broadcasted_iota(jnp.int32, (size, size), 1)
    line = lax.broadcasted_iota(jnp.int32, (size, size), 0)
    lane_row = lax.broadcasted_iota(jnp.int32, (1, size), 1)

    def step(p, carry):
        held = block[...]
        row = block[pl.ds(p, 1), :]
        pivot = 1.0 / jnp.sum(jnp.where(lane_row == p, row, 0.0), axis=1, keepdims=True)
        column = jnp.sum(jnp.where(lane == p, held, 0.0), axis=1, keepdims=True)
        scaled = jnp.where(lane_row == p, pivot, row * pivot)
        column = jnp.where(line[:, :1] == p, -1.0, column)
        kept = jnp.where((lane == p) | (line == p), 0.0, held)
        block[...] = kept - column * scaled
        return carry

    lax.fori_loop(0, size, step, 0)


def kernel(
    n, members, predicted, noise, observed, spread, out,
    pred_in, noise_in, cells_in, cells_out, relay, white, innov, part, part_in,
    sum_right, sum_left, in_right, in_left, total, table, pivots, weights, anomaly,
    own_sem, data_send, data_sem, in_send, in_sem, out_send, out_sem, pair_send, pair_sem,
    rs_send, rs_right, rs_left, ag_send, ag_right, ag_left, weight_send, weight_sem,
    relay_send, relay_sem, beside_send, relayed_send, own_out, known_left, known_right,
):
    nz = n // 2
    half = nz // 2
    me = lax.axis_index(ROWS)
    z, core = lax.div(me, 2), lax.rem(me, 2)
    local, cells = members.shape[0], members.shape[1] // n
    data = predicted.shape[1] // n
    count = n * local
    width = cells // CHUNKS
    scale = 1.0 / math.sqrt(count - 1)
    blocks = count // BLOCK
    lines = part.shape[0] // nz

    def remote(src, dst, send_sem, recv_sem, peer):
        pltpu.make_async_remote_copy(
            src_ref=src, dst_ref=dst, send_sem=send_sem, recv_sem=recv_sem,
            device_id={ROWS: peer}, device_id_type=MESH,
        ).start()

    def to_other_chips(send):
        def at(shift):
            for other in (0, 1):
                send(lax.rem(z + shift, nz) * 2 + lax.rem(core + other, 2))

        at(half)

        def both_ways(i, carry):
            at(half - i)
            at(half + i)
            return carry

        lax.fori_loop(1, half, both_ways, 0)

    def to_peers(send):
        to_other_chips(send)
        send(z * 2 + 1 - core)

    def span(index, size):
        return pl.ds(pl.multiple_of(index * size, 128), size)

    def piece(index, k):
        return pl.ds(pl.multiple_of(index * cells + k * width, 128), width)
    barrier = pltpu.get_barrier_semaphore()

    def chip(shift):
        return lax.rem(z + shift, nz) * 2

    def greet(semaphore, peer):
        pl.semaphore_signal(semaphore, inc=1, device_id={ROWS: peer}, device_id_type=MESH)

    for peer in (chip(0) + 1 - core, chip(1), chip(1) + 1, chip(nz - 1), chip(nz - 1) + 1):
        greet(barrier, peer)
    own_pred = pltpu.make_async_copy(predicted.at[:, span(me, data)], pred_in.at[me], own_sem.at[0])
    own_noise = pltpu.make_async_copy(noise.at[:, span(me, data)], noise_in.at[me], own_sem.at[1])
    own_cells = pltpu.make_async_copy(members.at[:, span(me, cells)], cells_in.at[me], own_sem.at[2])
    own_pred.start()
    own_noise.start()
    own_cells.start()
    pl.semaphore_wait(barrier, 5)

    def send_data(peer):
        remote(predicted.at[:, span(peer, data)], pred_in.at[me], data_send.at[0], data_sem.at[0], peer)
        remote(noise.at[:, span(peer, data)], noise_in.at[me], data_send.at[1], data_sem.at[1], peer)

    def send_cells(k):
        def send(peer):
            remote(members.at[:, piece(peer, k)], cells_in.at[me, :, piece(0, k)], in_send, in_sem.at[k], peer)

        to_peers(send)

    def pass_cells(k):
        def send(peer):
            remote(relay.at[:, piece(peer, k)], cells_in.at[me + 1, :, piece(0, k)], relayed_send, in_sem.at[k], peer)

        to_other_chips(send)
    send_data(chip(0) + 1 - core)

    def data_at(shift):
        for other in (0, 1):
            send_data(chip(shift) + lax.rem(core + other, 2))

    def widen(i, carry):
        greet(known_left.at[i - 1], chip(1) + core)
        greet(known_right.at[i - 1], chip(nz - 1) + core)

        @pl.when(i <= NEAR)
        def _():
            data_at(i)
            data_at(nz - i)

        pl.semaphore_wait(known_left.at[i - 1], 1)
        pl.semaphore_wait(known_right.at[i - 1], 1)
        return carry

    lax.fori_loop(1, half, widen, 0)
    data_at(half)

    def rest_of_data(i, carry):
        data_at(half - i)
        data_at(half + i)
        return carry

    lax.fori_loop(1, half - NEAR, rest_of_data, 0)

    @pl.when(core == 0)
    def _():
        send_cells(0)

    @pl.when(core == 1)
    def _():
        remote(members, relay, relay_send, relay_sem, me - 1)

        def beside(k, carry):
            remote(
                members.at[:, piece(me - 1, k)], cells_in.at[me, :, piece(0, k)], beside_send, in_sem.at[k], me - 1
            )
            return carry

        lax.fori_loop(0, RELAYED, beside, 0)
    own_pred.wait()
    own_noise.wait()
    drain(pred_in.at[pl.ds(0, n - 1)], data_sem.at[0])
    drain(noise_in.at[pl.ds(0, n - 1)], data_sem.at[1])

    def add_rows(i, acc):
        return acc + pred_in[i].astype(F32)

    sums = lax.fori_loop(0, n, add_rows, jnp.zeros((local, data), F32))
    mean = jnp.sum(sums, axis=0, keepdims=True) * (1.0 / count)
    spreads = spread[...]
    factor = scale / spreads
    target = observed[...]

    def standardize(i, carry):
        x = pred_in[pl.ds(2 * i, 2)].astype(F32).reshape(2 * local, data)
        e = noise_in[pl.ds(2 * i, 2)].astype(F32).reshape(2 * local, data)
        rows = pl.ds(pl.multiple_of(2 * local * i, 2 * local), 2 * local)
        white[rows, :] = ((x - mean) * factor).astype(BF16)
        innov[rows, :] = ((target - x) / spreads + e).astype(BF16)
        return carry

    lax.fori_loop(0, n // 2, standardize, 0)
    along = (((1,), (1,)), ((), ()))
    panels = []
    for i in range(blocks):
        start = sum(2 * blocks - k for k in range(i)) * BLOCK
        panels.append(start)
        rows = white[i * BLOCK : (i + 1) * BLOCK, :]
        gram = lax.dot_general(rows, white[i * BLOCK :, :], along, preferred_element_type=F32)
        cross = lax.dot_general(rows, innov[...], along, preferred_element_type=F32)
        for k in range(blocks - i):
            part[start + k * BLOCK : start + (k + 1) * BLOCK, :] = gram[:, k * BLOCK : (k + 1) * BLOCK]
        start += (blocks - i) * BLOCK
        for k in range(blocks):
            part[start + k * BLOCK : start + (k + 1) * BLOCK, :] = cross[:, k * BLOCK : (k + 1) * BLOCK]

    @pl.when(core == 0)
    def _():
        remote(part, part_in, pair_send, pair_sem, me + 1)
        drain(relay, relay_sem)

        def rest(k, carry):
            pass_cells(k)
            send_cells(k + 1)
            return carry

        lax.fori_loop(0, min(RELAYED, CHUNKS - 1), rest, 0)
        if RELAYED == CHUNKS:
            pass_cells(CHUNKS - 1)
        drain(part, pair_send)
        drain(weights, weight_sem)

    @pl.when(core == 1)
    def _():
        drain(part_in, pair_sem)
        right = lax.rem(z + 1, nz) * 2 + 1
        left = lax.rem(z + nz - 1, nz) * 2 + 1
        halves = halves_of(lines)

        def slab(j, start, size):
            return pl.ds(pl.multiple_of(j * lines + start, 8), size)

        def pair(j, h):
            return part[slab(j, *halves[h]), :] + part_in[slab(j, *halves[h]), :]

        def reduce_one(i, j, h, first, sums, landed, side, sems, peer):
            rows = pl.ds(*halves[h])
            value = pair(j, h)
            if not first:
                drain(landed.at[i - 1, rows], sems.at[h, i - 1])
                value = value + landed[i - 1, rows]
            sums[i, rows] = value
            remote(sums.at[i, rows], landed.at[i, rows], rs_send.at[side], sems.at[h, i], peer)

        def reduce_right(i, h, first=False):
            reduce_one(i, lax.rem(z + half + nz - i, nz), h, first, sum_right, in_right, 0, rs_right, right)

        def reduce_left(i, h, first=False):
            reduce_one(i, lax.rem(z + nz - half + 1 + i, nz), h, first, sum_left, in_left, 1, rs_left, left)

        for h in (0, 1):
            reduce_right(0, h, True)
            reduce_left(0, h, True)

        def reduce(i, carry):
            for h in (0, 1):
                reduce_right(i, h)
                reduce_left(i, h)
            return carry

        lax.fori_loop(1, half - 1, reduce, 0)
        for h in (0, 1):
            reduce_right(half - 1, h)
        for h in (0, 1):
            rows = pl.ds(*halves[h])
            drain(in_left.at[half - 2, rows], rs_left.at[h, half - 2])
            drain(in_right.at[half - 1, rows], rs_right.at[h, half - 1])
            total[slab(z, *halves[h]), :] = pair(z, h) + in_left[half - 2, rows] + in_right[half - 1, rows]

        def spread_one(i, j, h, first, side, sems, peer):
            rows = slab(j, *halves[h])
            if not first:
                drain(total.at[rows], sems.at[h, i - 1])
            remote(total.at[rows], total.at[rows], ag_send.at[side], sems.at[h, i], peer)

        def spread_right(i, h, first=False):
            spread_one(i, lax.rem(z + nz - i, nz), h, first, 0, ag_right, right)

        def spread_left(i, h, first=False):
            spread_one(i, lax.rem(z + i, nz), h, first, 1, ag_left, left)

        for h in (0, 1):
            spread_right(0, h, True)
            spread_left(0, h, True)

        def spread_on(i, carry):
            for h in (0, 1):
                spread_right(i, h)
                spread_left(i, h)
            return carry

        lax.fori_loop(1, half - 1, spread_on, 0)
        for h in (0, 1):
            spread_right(half - 1, h)
        for h in (0, 1):
            drain(total.at[pl.ds(0, halves[h][1])], ag_left.at[h, half - 2])
            drain(total.at[pl.ds(0, halves[h][1])], ag_right.at[h, half - 1])

        def rest(k, carry):
            send_cells(k)
            return carry

        lax.fori_loop(RELAYED, CHUNKS, rest, 0)
        for i in range(blocks):
            for k in range(2 * blocks - i):
                table[i * BLOCK : (i + 1) * BLOCK, (i + k) * BLOCK : (i + k + 1) * BLOCK] = total[
                    panels[i] + k * BLOCK : panels[i] + (k + 1) * BLOCK, :
                ]
        eye = lax.broadcasted_iota(jnp.int32, (BLOCK, BLOCK), 0) == lax.broadcasted_iota(
            jnp.int32, (BLOCK, BLOCK), 1
        )
        for k in range(blocks):
            here = slice(k * BLOCK, (k + 1) * BLOCK)
            ahead = slice((k + 1) * BLOCK, 2 * count)
            pivots[...] = table[here, here] + jnp.where(eye, DAMPING, 0.0)
            inverse_in_place(pivots)
            panel = table[here, ahead]
            scaled = exact_dot(pivots[...], panel)
            for i in range(k + 1, blocks):
                start = (i - k - 1) * BLOCK
                across = panel[:, start : start + BLOCK].T
                rows = slice(i * BLOCK, (i + 1) * BLOCK)
                table[rows, i * BLOCK :] = table[rows, i * BLOCK :] - exact_dot(across, scaled[:, start:])
            table[here, ahead] = scaled
        for k in reversed(range(blocks - 1)):
            here = slice(k * BLOCK, (k + 1) * BLOCK)
            table[here, count:] = table[here, count:] - exact_dot(
                table[here, (k + 1) * BLOCK : count], table[(k + 1) * BLOCK : count, count:]
            )
        for k in range(blocks):
            here = slice(k * BLOCK, (k + 1) * BLOCK)
            weights[:, here] = table[here, count:].T.astype(BF16)
        remote(weights, weights, weight_send, weight_sem, me - 1)

    own_cells.wait()

    def update(k, carry):
        columns = piece(0, k)
        drain(cells_in.at[pl.ds(0, n - 1), :, columns], in_sem.at[k])

        def add_cells(i, acc):
            return acc + cells_in[i, :, columns].astype(F32)

        sums = lax.fori_loop(0, n, add_cells, jnp.zeros((local, width), F32))
        mean = jnp.sum(sums, axis=0, keepdims=True) * (1.0 / count)

        def center(i, inner):
            x = cells_in[pl.ds(2 * i, 2), :, columns].astype(F32).reshape(2 * local, width)
            rows = pl.ds(pl.multiple_of(2 * local * i, 2 * local), 2 * local)
            anomaly[rows, :] = ((x - mean) * scale).astype(BF16)
            return inner

        lax.fori_loop(0, n // 2, center, 0)

        def renew(i, inner):
            rows = pl.ds(pl.multiple_of(BLOCK * i, BLOCK), BLOCK)
            slabs = pl.ds(i * (BLOCK // local), BLOCK // local)
            change = jnp.dot(weights[rows, :], anomaly[...], preferred_element_type=F32)
            x = cells_in[slabs, :, columns].astype(F32)
            cells_out[slabs, :, columns] = (x + change.reshape(x.shape)).astype(BF16)
            return inner

        lax.fori_loop(0, blocks, renew, 0)

        def send(peer):
            remote(cells_out.at[peer, :, columns], out.at[:, piece(me, k)], out_send, out_sem, peer)

        to_peers(send)
        return carry

    lax.fori_loop(0, CHUNKS, update, 0)
    mine = pltpu.make_async_copy(cells_out.at[me], out.at[:, span(me, cells)], own_out)
    mine.start()
    drain(pred_in.at[pl.ds(0, n - 1)], data_send.at[0])
    drain(noise_in.at[pl.ds(0, n - 1)], data_send.at[1])

    @pl.when(core == 0)
    def _():
        drain(cells_in.at[pl.ds(0, n - 1)], in_send)
        drain(cells_in.at[pl.ds(0, n - 2), :, pl.ds(0, RELAYED * width)], relayed_send)

    @pl.when(core == 1)
    def _():
        if RELAYED < CHUNKS:
            drain(cells_in.at[pl.ds(0, n - 1), :, pl.ds(0, (CHUNKS - RELAYED) * width)], in_send)
        drain(members, relay_send)
        drain(cells_in.at[0, :, pl.ds(0, RELAYED * width)], beside_send)
        drain(weights, weight_send)
        drain(total.at[pl.ds(0, half * lines)], rs_send.at[0])
        drain(total.at[pl.ds(0, (half - 1) * lines)], rs_send.at[1])
        drain(total.at[pl.ds(0, half * lines)], ag_send.at[0])
        drain(total.at[pl.ds(0, (half - 1) * lines)], ag_send.at[1])

    drain(cells_out.at[pl.ds(0, n - 1)], out_send)
    drain(cells_out.at[pl.ds(0, n - 1)], out_sem)
    mine.wait()


def solution(mesh):
    n = mesh.shape[ROWS]

    def on_device(members, predicted, noise, observed, spread):
        local = members.shape[0]
        count, nz = n * local, n // 2
        cells, data = members.shape[1] // n, predicted.shape[1] // n
        half, blocks = nz // 2, count // BLOCK
        packed = (blocks * (blocks + 1) // 2 + blocks * blocks) * BLOCK
        lines = packed // nz
        anywhere = pl.BlockSpec(memory_space=pltpu.HBM)
        on_chip = pl.BlockSpec(memory_space=pltpu.VMEM)
        dma = pltpu.SemaphoreType.DMA
        return pl.pallas_call(
            functools.partial(kernel, n),
            name="smoother",
            out_shape=jax.ShapeDtypeStruct(members.shape, members.dtype),
            in_specs=[anywhere, anywhere, anywhere, on_chip, on_chip],
            out_specs=anywhere,
            scratch_shapes=[
                pltpu.VMEM((n, local, data), BF16),
                pltpu.VMEM((n, local, data), BF16),
                pltpu.VMEM((n, local, cells), BF16),
                pltpu.VMEM((n, local, cells), BF16),
                pltpu.VMEM(members.shape, BF16),
                pltpu.VMEM((count, data), BF16),
                pltpu.VMEM((count, data), BF16),
                pltpu.VMEM((packed, BLOCK), F32),
                pltpu.VMEM((packed, BLOCK), F32),
                pltpu.VMEM((half, lines, BLOCK), F32),
                pltpu.VMEM((half, lines, BLOCK), F32),
                pltpu.VMEM((half, lines, BLOCK), F32),
                pltpu.VMEM((half, lines, BLOCK), F32),
                pltpu.VMEM((packed, BLOCK), F32),
                pltpu.VMEM((count, 2 * count), F32),
                pltpu.VMEM((BLOCK, BLOCK), F32),
                pltpu.VMEM((count, count), BF16),
                pltpu.VMEM((count, cells // CHUNKS), BF16),
                dma((3,)), dma((2,)), dma((2,)), dma, dma((CHUNKS,)), dma, dma, dma, dma,
                dma((2,)), dma((2, half)), dma((2, half)), dma((2,)), dma((2, half)), dma((2, half)),
                dma, dma, dma, dma, dma, dma, dma,
                pltpu.SemaphoreType.REGULAR((half - 1,)), pltpu.SemaphoreType.REGULAR((half - 1,)),
            ],
            compiler_params=pltpu.CompilerParams(collective_id=0, has_side_effects=True),
        )(members, predicted, noise, observed.reshape(1, data), spread.reshape(1, data))

    placed = (P(ROWS, "fields"), P(ROWS, "fields"), P(ROWS, "fields"), P(("fields", ROWS)), P(("fields", ROWS)))
    return jax.shard_map(
        on_device, mesh=mesh, in_specs=placed, out_specs=P(ROWS, "fields"), check_vma=False
    )
```

```python
import functools
import math

import jax
import jax.numpy as jnp
from jax import lax
from jax.experimental import pallas as pl
from jax.experimental.pallas import tpu as pltpu
from jax.sharding import PartitionSpec as P

ROWS = "rows"
MESH = pl.DeviceIdType.MESH
DAMPING = 21.0
CHUNKS = 4
RELAYED = 3
NEAR = 6
BLOCK = 128
F32 = jnp.float32
BF16 = jnp.bfloat16


def drain(ref, sem):
    pltpu.make_async_copy(ref, ref, sem).wait()


def exact_dot(a, b):
    return jnp.dot(a, b, precision=lax.Precision.HIGHEST, preferred_element_type=F32)


def halves_of(lines):
    first = (lines // 8 + 1) // 2 * 8
    return ((0, first), (first, lines - first))


def inverse_in_place(block):
    size = block.shape[0]
    lane = lax.broadcasted_iota(jnp.int32, (size, size), 1)
    line = lax.broadcasted_iota(jnp.int32, (size, size), 0)
    lane_row = lax.broadcasted_iota(jnp.int32, (1, size), 1)

    line_column = lax.broadcasted_iota(jnp.int32, (size, 1), 0)

    def across(mask, values):
        return jnp.sum(jnp.where(mask, values, 0.0), axis=1, keepdims=True)

    def step(i, carry):
        p, q = 2 * i, 2 * i + 1
        held = block[...]
        row_p, row_q = block[pl.ds(p, 1), :], block[pl.ds(q, 1), :]
        at_p, at_q = lane_row == p, lane_row == q
        corner, beside = across(at_q, row_p), across(at_p, row_q)
        pivot_p = 1.0 / across(at_p, row_p)
        ratio = corner * pivot_p
        pivot_q = 1.0 / (across(at_q, row_q) - beside * ratio)
        scaled_p = jnp.where(at_p, pivot_p, row_p * pivot_p)
        scaled_q = (jnp.where(at_p, 0.0, row_q) - beside * scaled_p) * pivot_q
        scaled_q = jnp.where(at_q, pivot_q, scaled_q)
        column_p = jnp.where(line_column == p, -1.0, across(lane == p, held))
        column_q = jnp.where(line_column == p, 0.0, across(lane == q, held)) - column_p * ratio
        column_q = jnp.where(line_column == q, -1.0, column_q)
        kept = jnp.where((lane == p) | (line == p), 0.0, held) - column_p * scaled_p
        block[...] = jnp.where((lane == q) | (line == q), 0.0, kept) - column_q * scaled_q
        return carry

    lax.fori_loop(0, size // 2, step, 0)


def kernel(
    n, members, predicted, noise, observed, spread, out,
    pred_in, noise_in, cells_in, cells_out, relay, white, innov, part, part_in,
    sum_right, sum_left, in_right, in_left, total, table, pivots, weights, anomaly,
    own_sem, data_send, data_sem, in_send, in_sem, out_send, out_sem, pair_send, pair_sem,
    rs_send, rs_right, rs_left, ag_send, ag_right, ag_left, weight_send, weight_sem,
    relay_send, relay_sem, beside_send, relayed_send, own_out, known_left, known_right,
):
    nz = n // 2
    half = nz // 2
    me = lax.axis_index(ROWS)
    z, core = lax.div(me, 2), lax.rem(me, 2)
    local, cells = members.shape[0], members.shape[1] // n
    data = predicted.shape[1] // n
    count = n * local
    width = cells // CHUNKS
    scale = 1.0 / math.sqrt(count - 1)
    blocks = count // BLOCK
    lines = part.shape[0] // nz

    def remote(src, dst, send_sem, recv_sem, peer):
        pltpu.make_async_remote_copy(
            src_ref=src, dst_ref=dst, send_sem=send_sem, recv_sem=recv_sem,
            device_id={ROWS: peer}, device_id_type=MESH,
        ).start()

    def to_other_chips(send):
        def at(shift):
            for other in (0, 1):
                send(lax.rem(z + shift, nz) * 2 + lax.rem(core + other, 2))

        at(half)

        def both_ways(i, carry):
            at(half - i)
            at(half + i)
            return carry

        lax.fori_loop(1, half, both_ways, 0)

    def to_peers(send):
        to_other_chips(send)
        send(z * 2 + 1 - core)

    def span(index, size):
        return pl.ds(pl.multiple_of(index * size, 128), size)

    def piece(index, k):
        return pl.ds(pl.multiple_of(index * cells + k * width, 128), width)
    barrier = pltpu.get_barrier_semaphore()

    def chip(shift):
        return lax.rem(z + shift, nz) * 2

    def greet(semaphore, peer):
        pl.semaphore_signal(semaphore, inc=1, device_id={ROWS: peer}, device_id_type=MESH)

    for peer in (chip(0) + 1 - core, chip(1), chip(1) + 1, chip(nz - 1), chip(nz - 1) + 1):
        greet(barrier, peer)
    own_pred = pltpu.make_async_copy(predicted.at[:, span(me, data)], pred_in.at[me], own_sem.at[0])
    own_noise = pltpu.make_async_copy(noise.at[:, span(me, data)], noise_in.at[me], own_sem.at[1])
    own_cells = pltpu.make_async_copy(members.at[:, span(me, cells)], cells_in.at[me], own_sem.at[2])
    own_pred.start()
    own_noise.start()
    own_cells.start()
    pl.semaphore_wait(barrier, 5)

    def send_data(peer):
        remote(predicted.at[:, span(peer, data)], pred_in.at[me], data_send.at[0], data_sem.at[0], peer)
        remote(noise.at[:, span(peer, data)], noise_in.at[me], data_send.at[1], data_sem.at[1], peer)

    def send_cells(k):
        def send(peer):
            remote(members.at[:, piece(peer, k)], cells_in.at[me, :, piece(0, k)], in_send, in_sem.at[k], peer)

        to_peers(send)

    def pass_cells(k):
        def send(peer):
            remote(relay.at[:, piece(peer, k)], cells_in.at[me + 1, :, piece(0, k)], relayed_send, in_sem.at[k], peer)

        to_other_chips(send)
    send_data(chip(0) + 1 - core)

    def data_at(shift):
        for other in (0, 1):
            send_data(chip(shift) + lax.rem(core + other, 2))

    def widen(i, carry):
        greet(known_left.at[i - 1], chip(1) + core)
        greet(known_right.at[i - 1], chip(nz - 1) + core)

        @pl.when(i <= NEAR)
        def _():
            data_at(i)
            data_at(nz - i)

        pl.semaphore_wait(known_left.at[i - 1], 1)
        pl.semaphore_wait(known_right.at[i - 1], 1)
        return carry

    lax.fori_loop(1, half, widen, 0)
    data_at(half)

    def rest_of_data(i, carry):
        data_at(half - i)
        data_at(half + i)
        return carry

    lax.fori_loop(1, half - NEAR, rest_of_data, 0)

    @pl.when(core == 0)
    def _():
        send_cells(0)

    @pl.when(core == 1)
    def _():
        remote(members, relay, relay_send, relay_sem, me - 1)

        def beside(k, carry):
            remote(
                members.at[:, piece(me - 1, k)], cells_in.at[me, :, piece(0, k)], beside_send, in_sem.at[k], me - 1
            )
            return carry

        lax.fori_loop(0, RELAYED, beside, 0)
    own_pred.wait()
    own_noise.wait()
    drain(pred_in.at[pl.ds(0, n - 1)], data_sem.at[0])
    drain(noise_in.at[pl.ds(0, n - 1)], data_sem.at[1])

    def add_rows(i, acc):
        return acc + pred_in[i].astype(F32)

    sums = lax.fori_loop(0, n, add_rows, jnp.zeros((local, data), F32))
    mean = jnp.sum(sums, axis=0, keepdims=True) * (1.0 / count)
    spreads = spread[...]
    factor = scale / spreads
    target = observed[...]

    def standardize(i, carry):
        x = pred_in[pl.ds(2 * i, 2)].astype(F32).reshape(2 * local, data)
        e = noise_in[pl.ds(2 * i, 2)].astype(F32).reshape(2 * local, data)
        rows = pl.ds(pl.multiple_of(2 * local * i, 2 * local), 2 * local)
        white[rows, :] = ((x - mean) * factor).astype(BF16)
        innov[rows, :] = ((target - x) / spreads + e).astype(BF16)
        return carry

    lax.fori_loop(0, n // 2, standardize, 0)
    along = (((1,), (1,)), ((), ()))
    panels = []
    for i in range(blocks):
        start = sum(2 * blocks - k for k in range(i)) * BLOCK
        panels.append(start)
        rows = white[i * BLOCK : (i + 1) * BLOCK, :]
        gram = lax.dot_general(rows, white[i * BLOCK :, :], along, preferred_element_type=F32)
        cross = lax.dot_general(rows, innov[...], along, preferred_element_type=F32)
        for k in range(blocks - i):
            part[start + k * BLOCK : start + (k + 1) * BLOCK, :] = gram[:, k * BLOCK : (k + 1) * BLOCK]
        start += (blocks - i) * BLOCK
        for k in range(blocks):
            part[start + k * BLOCK : start + (k + 1) * BLOCK, :] = cross[:, k * BLOCK : (k + 1) * BLOCK]

    @pl.when(core == 0)
    def _():
        remote(part, part_in, pair_send, pair_sem, me + 1)
        drain(relay, relay_sem)

        def rest(k, carry):
            pass_cells(k)
            send_cells(k + 1)
            return carry

        lax.fori_loop(0, min(RELAYED, CHUNKS - 1), rest, 0)
        if RELAYED == CHUNKS:
            pass_cells(CHUNKS - 1)
        drain(part, pair_send)
        drain(weights, weight_sem)

    @pl.when(core == 1)
    def _():
        drain(part_in, pair_sem)
        right = lax.rem(z + 1, nz) * 2 + 1
        left = lax.rem(z + nz - 1, nz) * 2 + 1
        halves = halves_of(lines)

        def slab(j, start, size):
            return pl.ds(pl.multiple_of(j * lines + start, 8), size)

        def pair(j, h):
            return part[slab(j, *halves[h]), :] + part_in[slab(j, *halves[h]), :]

        def reduce_one(i, j, h, first, sums, landed, side, sems, peer):
            rows = pl.ds(*halves[h])
            value = pair(j, h)
            if not first:
                drain(landed.at[i - 1, rows], sems.at[h, i - 1])
                value = value + landed[i - 1, rows]
            sums[i, rows] = value
            remote(sums.at[i, rows], landed.at[i, rows], rs_send.at[side], sems.at[h, i], peer)

        def reduce_right(i, h, first=False):
            reduce_one(i, lax.rem(z + half + nz - i, nz), h, first, sum_right, in_right, 0, rs_right, right)

        def reduce_left(i, h, first=False):
            reduce_one(i, lax.rem(z + nz - half + 1 + i, nz), h, first, sum_left, in_left, 1, rs_left, left)

        for h in (0, 1):
            reduce_right(0, h, True)
            reduce_left(0, h, True)

        def reduce(i, carry):
            for h in (0, 1):
                reduce_right(i, h)
                reduce_left(i, h)
            return carry

        lax.fori_loop(1, half - 1, reduce, 0)
        for h in (0, 1):
            reduce_right(half - 1, h)
        for h in (0, 1):
            rows = pl.ds(*halves[h])
            drain(in_left.at[half - 2, rows], rs_left.at[h, half - 2])
            drain(in_right.at[half - 1, rows], rs_right.at[h, half - 1])
            total[slab(z, *halves[h]), :] = pair(z, h) + in_left[half - 2, rows] + in_right[half - 1, rows]

        def spread_one(i, j, h, first, side, sems, peer):
            rows = slab(j, *halves[h])
            if not first:
                drain(total.at[rows], sems.at[h, i - 1])
            remote(total.at[rows], total.at[rows], ag_send.at[side], sems.at[h, i], peer)

        def spread_right(i, h, first=False):
            spread_one(i, lax.rem(z + nz - i, nz), h, first, 0, ag_right, right)

        def spread_left(i, h, first=False):
            spread_one(i, lax.rem(z + i, nz), h, first, 1, ag_left, left)

        for h in (0, 1):
            spread_right(0, h, True)
            spread_left(0, h, True)

        def spread_on(i, carry):
            for h in (0, 1):
                spread_right(i, h)
                spread_left(i, h)
            return carry

        lax.fori_loop(1, half - 1, spread_on, 0)
        for h in (0, 1):
            spread_right(half - 1, h)
        for h in (0, 1):
            drain(total.at[pl.ds(0, halves[h][1])], ag_left.at[h, half - 2])
            drain(total.at[pl.ds(0, halves[h][1])], ag_right.at[h, half - 1])

        def rest(k, carry):
            send_cells(k)
            return carry

        lax.fori_loop(RELAYED, CHUNKS, rest, 0)
        for i in range(blocks):
            for k in range(2 * blocks - i):
                table[i * BLOCK : (i + 1) * BLOCK, (i + k) * BLOCK : (i + k + 1) * BLOCK] = total[
                    panels[i] + k * BLOCK : panels[i] + (k + 1) * BLOCK, :
                ]
        eye = lax.broadcasted_iota(jnp.int32, (BLOCK, BLOCK), 0) == lax.broadcasted_iota(
            jnp.int32, (BLOCK, BLOCK), 1
        )
        for k in range(blocks):
            here = slice(k * BLOCK, (k + 1) * BLOCK)
            ahead = slice((k + 1) * BLOCK, 2 * count)
            pivots[...] = table[here, here] + jnp.where(eye, DAMPING, 0.0)
            inverse_in_place(pivots)
            panel = table[here, ahead]
            scaled = exact_dot(pivots[...], panel)
            for i in range(k + 1, blocks):
                start = (i - k - 1) * BLOCK
                across = panel[:, start : start + BLOCK].T
                rows = slice(i * BLOCK, (i + 1) * BLOCK)
                table[rows, i * BLOCK :] = table[rows, i * BLOCK :] - exact_dot(across, scaled[:, start:])
            table[here, ahead] = scaled
        for k in reversed(range(blocks - 1)):
            here = slice(k * BLOCK, (k + 1) * BLOCK)
            table[here, count:] = table[here, count:] - exact_dot(
                table[here, (k + 1) * BLOCK : count], table[(k + 1) * BLOCK : count, count:]
            )
        for k in range(blocks):
            here = slice(k * BLOCK, (k + 1) * BLOCK)
            weights[:, here] = table[here, count:].T.astype(BF16)
        remote(weights, weights, weight_send, weight_sem, me - 1)

    own_cells.wait()

    def update(k, carry):
        columns = piece(0, k)
        drain(cells_in.at[pl.ds(0, n - 1), :, columns], in_sem.at[k])

        def add_cells(i, acc):
            return acc + cells_in[i, :, columns].astype(F32)

        sums = lax.fori_loop(0, n, add_cells, jnp.zeros((local, width), F32))
        mean = jnp.sum(sums, axis=0, keepdims=True) * (1.0 / count)

        def center(i, inner):
            x = cells_in[pl.ds(2 * i, 2), :, columns].astype(F32).reshape(2 * local, width)
            rows = pl.ds(pl.multiple_of(2 * local * i, 2 * local), 2 * local)
            anomaly[rows, :] = ((x - mean) * scale).astype(BF16)
            return inner

        lax.fori_loop(0, n // 2, center, 0)

        def renew(i, inner):
            rows = pl.ds(pl.multiple_of(BLOCK * i, BLOCK), BLOCK)
            slabs = pl.ds(i * (BLOCK // local), BLOCK // local)
            change = jnp.dot(weights[rows, :], anomaly[...], preferred_element_type=F32)
            x = cells_in[slabs, :, columns].astype(F32)
            cells_out[slabs, :, columns] = (x + change.reshape(x.shape)).astype(BF16)
            return inner

        lax.fori_loop(0, blocks, renew, 0)

        def send(peer):
            remote(cells_out.at[peer, :, columns], out.at[:, piece(me, k)], out_send, out_sem, peer)

        to_peers(send)
        return carry

    lax.fori_loop(0, CHUNKS, update, 0)
    mine = pltpu.make_async_copy(cells_out.at[me], out.at[:, span(me, cells)], own_out)
    mine.start()
    drain(pred_in.at[pl.ds(0, n - 1)], data_send.at[0])
    drain(noise_in.at[pl.ds(0, n - 1)], data_send.at[1])

    @pl.when(core == 0)
    def _():
        drain(cells_in.at[pl.ds(0, n - 1)], in_send)
        drain(cells_in.at[pl.ds(0, n - 2), :, pl.ds(0, RELAYED * width)], relayed_send)

    @pl.when(core == 1)
    def _():
        if RELAYED < CHUNKS:
            drain(cells_in.at[pl.ds(0, n - 1), :, pl.ds(0, (CHUNKS - RELAYED) * width)], in_send)
        drain(members, relay_send)
        drain(cells_in.at[0, :, pl.ds(0, RELAYED * width)], beside_send)
        drain(weights, weight_send)
        drain(total.at[pl.ds(0, half * lines)], rs_send.at[0])
        drain(total.at[pl.ds(0, (half - 1) * lines)], rs_send.at[1])
        drain(total.at[pl.ds(0, half * lines)], ag_send.at[0])
        drain(total.at[pl.ds(0, (half - 1) * lines)], ag_send.at[1])

    drain(cells_out.at[pl.ds(0, n - 1)], out_send)
    drain(cells_out.at[pl.ds(0, n - 1)], out_sem)
    mine.wait()


def solution(mesh):
    n = mesh.shape[ROWS]

    def on_device(members, predicted, noise, observed, spread):
        local = members.shape[0]
        count, nz = n * local, n // 2
        cells, data = members.shape[1] // n, predicted.shape[1] // n
        half, blocks = nz // 2, count // BLOCK
        packed = (blocks * (blocks + 1) // 2 + blocks * blocks) * BLOCK
        lines = packed // nz
        anywhere = pl.BlockSpec(memory_space=pltpu.HBM)
        on_chip = pl.BlockSpec(memory_space=pltpu.VMEM)
        dma = pltpu.SemaphoreType.DMA
        return pl.pallas_call(
            functools.partial(kernel, n),
            name="smoother",
            out_shape=jax.ShapeDtypeStruct(members.shape, members.dtype),
            in_specs=[anywhere, anywhere, anywhere, on_chip, on_chip],
            out_specs=anywhere,
            scratch_shapes=[
                pltpu.VMEM((n, local, data), BF16),
                pltpu.VMEM((n, local, data), BF16),
                pltpu.VMEM((n, local, cells), BF16),
                pltpu.VMEM((n, local, cells), BF16),
                pltpu.VMEM(members.shape, BF16),
                pltpu.VMEM((count, data), BF16),
                pltpu.VMEM((count, data), BF16),
                pltpu.VMEM((packed, BLOCK), F32),
                pltpu.VMEM((packed, BLOCK), F32),
                pltpu.VMEM((half, lines, BLOCK), F32),
                pltpu.VMEM((half, lines, BLOCK), F32),
                pltpu.VMEM((half, lines, BLOCK), F32),
                pltpu.VMEM((half, lines, BLOCK), F32),
                pltpu.VMEM((packed, BLOCK), F32),
                pltpu.VMEM((count, 2 * count), F32),
                pltpu.VMEM((BLOCK, BLOCK), F32),
                pltpu.VMEM((count, count), BF16),
                pltpu.VMEM((count, cells // CHUNKS), BF16),
                dma((3,)), dma((2,)), dma((2,)), dma, dma((CHUNKS,)), dma, dma, dma, dma,
                dma((2,)), dma((2, half)), dma((2, half)), dma((2,)), dma((2, half)), dma((2, half)),
                dma, dma, dma, dma, dma, dma, dma,
                pltpu.SemaphoreType.REGULAR((half - 1,)), pltpu.SemaphoreType.REGULAR((half - 1,)),
            ],
            compiler_params=pltpu.CompilerParams(collective_id=0, has_side_effects=True),
        )(members, predicted, noise, observed.reshape(1, data), spread.reshape(1, data))

    placed = (P(ROWS, "fields"), P(ROWS, "fields"), P(ROWS, "fields"), P(("fields", ROWS)), P(("fields", ROWS)))
    return jax.shard_map(
        on_device, mesh=mesh, in_specs=placed, out_specs=P(ROWS, "fields"), check_vma=False
    )
```

```python
import functools
import math

import jax
import jax.numpy as jnp
from jax import lax
from jax.experimental import pallas as pl
from jax.experimental.pallas import tpu as pltpu
from jax.sharding import PartitionSpec as P

ROWS = "rows"
MESH = pl.DeviceIdType.MESH
DAMPING = 21.0
CHUNKS = 4
RELAYED = 3
NEAR = 6
BLOCK = 128
F32 = jnp.float32
BF16 = jnp.bfloat16


def drain(ref, sem):
    pltpu.make_async_copy(ref, ref, sem).wait()


def exact_dot(a, b):
    return jnp.dot(a, b, precision=lax.Precision.HIGHEST, preferred_element_type=F32)


def halves_of(lines):
    first = (lines // 8 + 1) // 2 * 8
    return ((0, first), (first, lines - first))


def inverse_in_place(block):
    size = block.shape[0]
    lane = lax.broadcasted_iota(jnp.int32, (size, size), 1)
    line = lax.broadcasted_iota(jnp.int32, (size, size), 0)
    lane_row = lax.broadcasted_iota(jnp.int32, (1, size), 1)

    line_column = lax.broadcasted_iota(jnp.int32, (size, 1), 0)

    def across(mask, values):
        return jnp.sum(jnp.where(mask, values, 0.0), axis=1, keepdims=True)

    def step(i, carry):
        p, q = 2 * i, 2 * i + 1
        held = block[...]
        row_p, row_q = block[pl.ds(p, 1), :], block[pl.ds(q, 1), :]
        at_p, at_q = lane_row == p, lane_row == q
        corner, beside = across(at_q, row_p), across(at_p, row_q)
        pivot_p = 1.0 / across(at_p, row_p)
        ratio = corner * pivot_p
        pivot_q = 1.0 / (across(at_q, row_q) - beside * ratio)
        scaled_p = jnp.where(at_p, pivot_p, row_p * pivot_p)
        scaled_q = (jnp.where(at_p, 0.0, row_q) - beside * scaled_p) * pivot_q
        scaled_q = jnp.where(at_q, pivot_q, scaled_q)
        column_p = jnp.where(line_column == p, -1.0, across(lane == p, held))
        column_q = jnp.where(line_column == p, 0.0, across(lane == q, held)) - column_p * ratio
        column_q = jnp.where(line_column == q, -1.0, column_q)
        kept = jnp.where((lane == p) | (line == p), 0.0, held) - column_p * scaled_p
        block[...] = jnp.where((lane == q) | (line == q), 0.0, kept) - column_q * scaled_q
        return carry

    lax.fori_loop(0, size // 2, step, 0)


def kernel(
    n, members, predicted, noise, observed, spread, out,
    pred_in, noise_in, cells_in, cells_out, relay, white, innov, part, part_in,
    sum_right, sum_left, in_right, in_left, total, table, pivots, weights, anomaly,
    own_sem, data_send, data_sem, in_send, in_sem, out_send, out_sem, pair_send, pair_sem,
    rs_send, rs_right, rs_left, ag_send, ag_right, ag_left, weight_send, weight_sem,
    relay_send, relay_sem, beside_send, relayed_send, own_out, known_left, known_right,
):
    nz = n // 2
    half = nz // 2
    me = lax.axis_index(ROWS)
    z, core = lax.div(me, 2), lax.rem(me, 2)
    local, cells = members.shape[0], members.shape[1] // n
    data = predicted.shape[1] // n
    count = n * local
    width = cells // CHUNKS
    scale = 1.0 / math.sqrt(count - 1)
    blocks = count // BLOCK
    lines = part.shape[0] // nz

    def remote(src, dst, send_sem, recv_sem, peer):
        pltpu.make_async_remote_copy(
            src_ref=src, dst_ref=dst, send_sem=send_sem, recv_sem=recv_sem,
            device_id={ROWS: peer}, device_id_type=MESH,
        ).start()

    def to_other_chips(send):
        def at(shift):
            for other in (0, 1):
                send(lax.rem(z + shift, nz) * 2 + lax.rem(core + other, 2))

        at(half)

        def both_ways(i, carry):
            at(half - i)
            at(half + i)
            return carry

        lax.fori_loop(1, half, both_ways, 0)

    def to_peers(send):
        to_other_chips(send)
        send(z * 2 + 1 - core)

    def span(index, size):
        return pl.ds(pl.multiple_of(index * size, 128), size)

    def piece(index, k):
        return pl.ds(pl.multiple_of(index * cells + k * width, 128), width)
    barrier = pltpu.get_barrier_semaphore()

    def chip(shift):
        return lax.rem(z + shift, nz) * 2

    def greet(semaphore, peer):
        pl.semaphore_signal(semaphore, inc=1, device_id={ROWS: peer}, device_id_type=MESH)

    for peer in (chip(0) + 1 - core, chip(1), chip(1) + 1, chip(nz - 1), chip(nz - 1) + 1):
        greet(barrier, peer)
    own_pred = pltpu.make_async_copy(predicted.at[:, span(me, data)], pred_in.at[me], own_sem.at[0])
    own_noise = pltpu.make_async_copy(noise.at[:, span(me, data)], noise_in.at[me], own_sem.at[1])
    own_cells = pltpu.make_async_copy(members.at[:, span(me, cells)], cells_in.at[me], own_sem.at[2])
    own_pred.start()
    own_noise.start()
    own_cells.start()
    pl.semaphore_wait(barrier, 5)

    def send_data(peer):
        remote(predicted.at[:, span(peer, data)], pred_in.at[me], data_send.at[0], data_sem.at[0], peer)
        remote(noise.at[:, span(peer, data)], noise_in.at[me], data_send.at[1], data_sem.at[1], peer)

    def send_cells(k):
        def send(peer):
            remote(members.at[:, piece(peer, k)], cells_in.at[me, :, piece(0, k)], in_send, in_sem.at[k], peer)

        to_peers(send)

    def pass_cells(k):
        def send(peer):
            remote(relay.at[:, piece(peer, k)], cells_in.at[me + 1, :, piece(0, k)], relayed_send, in_sem.at[k], peer)

        to_other_chips(send)
    send_data(chip(0) + 1 - core)

    def data_at(shift):
        for other in (0, 1):
            send_data(chip(shift) + lax.rem(core + other, 2))

    def widen(i, carry):
        greet(known_left.at[i - 1], chip(1) + core)
        greet(known_right.at[i - 1], chip(nz - 1) + core)

        @pl.when(i <= NEAR)
        def _():
            data_at(i)
            data_at(nz - i)

        pl.semaphore_wait(known_left.at[i - 1], 1)
        pl.semaphore_wait(known_right.at[i - 1], 1)
        return carry

    lax.fori_loop(1, half, widen, 0)
    data_at(half)

    def rest_of_data(i, carry):
        data_at(half - i)
        data_at(half + i)
        return carry

    lax.fori_loop(1, half - NEAR, rest_of_data, 0)

    @pl.when(core == 0)
    def _():
        send_cells(0)

    @pl.when(core == 1)
    def _():
        remote(members, relay, relay_send, relay_sem, me - 1)

        def beside(k, carry):
            remote(
                members.at[:, piece(me - 1, k)], cells_in.at[me, :, piece(0, k)], beside_send, in_sem.at[k], me - 1
            )
            return carry

        lax.fori_loop(0, RELAYED, beside, 0)
    own_pred.wait()
    own_noise.wait()
    drain(pred_in.at[pl.ds(0, n - 1)], data_sem.at[0])
    drain(noise_in.at[pl.ds(0, n - 1)], data_sem.at[1])

    def add_rows(i, acc):
        return acc + pred_in[i].astype(F32)

    sums = lax.fori_loop(0, n, add_rows, jnp.zeros((local, data), F32))
    mean = jnp.sum(sums, axis=0, keepdims=True) * (1.0 / count)
    spreads = spread[...]
    factor = scale / spreads
    target = observed[...]

    def standardize(i, carry):
        x = pred_in[pl.ds(2 * i, 2)].astype(F32).reshape(2 * local, data)
        e = noise_in[pl.ds(2 * i, 2)].astype(F32).reshape(2 * local, data)
        rows = pl.ds(pl.multiple_of(2 * local * i, 2 * local), 2 * local)
        white[rows, :] = ((x - mean) * factor).astype(BF16)
        innov[rows, :] = ((target - x) / spreads + e).astype(BF16)
        return carry

    lax.fori_loop(0, n // 2, standardize, 0)
    along = (((1,), (1,)), ((), ()))
    panels = []
    for i in range(blocks):
        start = sum(2 * blocks - k for k in range(i)) * BLOCK
        panels.append(start)
        rows = white[i * BLOCK : (i + 1) * BLOCK, :]
        gram = lax.dot_general(rows, white[i * BLOCK :, :], along, preferred_element_type=F32)
        cross = lax.dot_general(rows, innov[...], along, preferred_element_type=F32)
        for k in range(blocks - i):
            part[start + k * BLOCK : start + (k + 1) * BLOCK, :] = gram[:, k * BLOCK : (k + 1) * BLOCK]
        start += (blocks - i) * BLOCK
        for k in range(blocks):
            part[start + k * BLOCK : start + (k + 1) * BLOCK, :] = cross[:, k * BLOCK : (k + 1) * BLOCK]

    @pl.when(core == 0)
    def _():
        remote(part, part_in, pair_send, pair_sem, me + 1)
        drain(relay, relay_sem)

        def rest(k, carry):
            pass_cells(k)
            send_cells(k + 1)
            return carry

        lax.fori_loop(0, min(RELAYED, CHUNKS - 1), rest, 0)
        if RELAYED == CHUNKS:
            pass_cells(CHUNKS - 1)
        drain(part, pair_send)
        drain(weights, weight_sem)

    @pl.when(core == 1)
    def _():
        drain(part_in, pair_sem)
        right = lax.rem(z + 1, nz) * 2 + 1
        left = lax.rem(z + nz - 1, nz) * 2 + 1
        halves = halves_of(lines)

        def slab(j, start, size):
            return pl.ds(pl.multiple_of(j * lines + start, 8), size)

        def pair(j, h):
            return part[slab(j, *halves[h]), :] + part_in[slab(j, *halves[h]), :]

        def reduce_one(i, j, h, first, sums, landed, side, sems, peer):
            rows = pl.ds(*halves[h])
            value = pair(j, h)
            if not first:
                drain(landed.at[i - 1, rows], sems.at[h, i - 1])
                value = value + landed[i - 1, rows]
            sums[i, rows] = value
            remote(sums.at[i, rows], landed.at[i, rows], rs_send.at[side], sems.at[h, i], peer)

        def reduce_right(i, h, first=False):
            reduce_one(i, lax.rem(z + half + nz - i, nz), h, first, sum_right, in_right, 0, rs_right, right)

        def reduce_left(i, h, first=False):
            reduce_one(i, lax.rem(z + nz - half + 1 + i, nz), h, first, sum_left, in_left, 1, rs_left, left)

        for h in (0, 1):
            reduce_right(0, h, True)
            reduce_left(0, h, True)

        def reduce(i, carry):
            for h in (0, 1):
                reduce_right(i, h)
                reduce_left(i, h)
            return carry

        lax.fori_loop(1, half - 1, reduce, 0)
        for h in (0, 1):
            reduce_right(half - 1, h)
        for h in (0, 1):
            rows = pl.ds(*halves[h])
            drain(in_left.at[half - 2, rows], rs_left.at[h, half - 2])
            drain(in_right.at[half - 1, rows], rs_right.at[h, half - 1])
            total[slab(z, *halves[h]), :] = pair(z, h) + in_left[half - 2, rows] + in_right[half - 1, rows]

        def spread_one(i, j, h, first, side, sems, peer):
            rows = slab(j, *halves[h])
            if not first:
                drain(total.at[rows], sems.at[h, i - 1])
            remote(total.at[rows], total.at[rows], ag_send.at[side], sems.at[h, i], peer)

        def spread_right(i, h, first=False):
            spread_one(i, lax.rem(z + nz - i, nz), h, first, 0, ag_right, right)

        def spread_left(i, h, first=False):
            spread_one(i, lax.rem(z + i, nz), h, first, 1, ag_left, left)

        for h in (0, 1):
            spread_right(0, h, True)
            spread_left(0, h, True)

        def spread_on(i, carry):
            for h in (0, 1):
                spread_right(i, h)
                spread_left(i, h)
            return carry

        lax.fori_loop(1, half - 1, spread_on, 0)
        for h in (0, 1):
            spread_right(half - 1, h)
        for h in (0, 1):
            drain(total.at[pl.ds(0, halves[h][1])], ag_left.at[h, half - 2])
            drain(total.at[pl.ds(0, halves[h][1])], ag_right.at[h, half - 1])

        def rest(k, carry):
            send_cells(k)
            return carry

        lax.fori_loop(RELAYED, CHUNKS, rest, 0)
        for i in range(blocks):
            for k in range(2 * blocks - i):
                table[i * BLOCK : (i + 1) * BLOCK, (i + k) * BLOCK : (i + k + 1) * BLOCK] = total[
                    panels[i] + k * BLOCK : panels[i] + (k + 1) * BLOCK, :
                ]
        eye = lax.broadcasted_iota(jnp.int32, (BLOCK, BLOCK), 0) == lax.broadcasted_iota(
            jnp.int32, (BLOCK, BLOCK), 1
        )
        for k in range(blocks):
            here = slice(k * BLOCK, (k + 1) * BLOCK)
            ahead = slice((k + 1) * BLOCK, 2 * count)
            pivots[...] = table[here, here] + jnp.where(eye, DAMPING, 0.0)
            inverse_in_place(pivots)
            panel = table[here, ahead]
            scaled = exact_dot(pivots[...], panel)
            for i in range(k + 1, blocks):
                start = (i - k - 1) * BLOCK
                across = panel[:, start : start + BLOCK].T
                rows = slice(i * BLOCK, (i + 1) * BLOCK)
                table[rows, i * BLOCK :] = table[rows, i * BLOCK :] - exact_dot(across, scaled[:, start:])
            table[here, ahead] = scaled
        for k in reversed(range(blocks - 1)):
            here = slice(k * BLOCK, (k + 1) * BLOCK)
            table[here, count:] = table[here, count:] - exact_dot(
                table[here, (k + 1) * BLOCK : count], table[(k + 1) * BLOCK : count, count:]
            )
        for k in range(blocks):
            here = slice(k * BLOCK, (k + 1) * BLOCK)
            weights[:, here] = table[here, count:].T.astype(BF16)
        remote(weights, weights, weight_send, weight_sem, me - 1)

    own_cells.wait()

    def update(k, carry):
        columns = piece(0, k)
        drain(cells_in.at[pl.ds(0, n - 1), :, columns], in_sem.at[k])

        def add_cells(i, acc):
            return acc + cells_in[i, :, columns].astype(F32)

        sums = lax.fori_loop(0, n, add_cells, jnp.zeros((local, width), F32))
        mean = jnp.sum(sums, axis=0, keepdims=True) * (1.0 / count)

        def center(i, inner):
            x = cells_in[pl.ds(2 * i, 2), :, columns].astype(F32).reshape(2 * local, width)
            rows = pl.ds(pl.multiple_of(2 * local * i, 2 * local), 2 * local)
            anomaly[rows, :] = ((x - mean) * scale).astype(BF16)
            return inner

        lax.fori_loop(0, n // 2, center, 0)

        def renew(i, inner):
            rows = pl.ds(pl.multiple_of(BLOCK * i, BLOCK), BLOCK)
            slabs = pl.ds(i * (BLOCK // local), BLOCK // local)
            change = jnp.dot(weights[rows, :], anomaly[...], preferred_element_type=F32)
            x = cells_in[slabs, :, columns].astype(F32)
            cells_out[slabs, :, columns] = (x + change.reshape(x.shape)).astype(BF16)
            return inner

        lax.fori_loop(0, blocks, renew, 0)

        def send(peer):
            remote(cells_out.at[peer, :, columns], out.at[:, piece(me, k)], out_send, out_sem, peer)

        to_peers(send)
        return carry

    lax.fori_loop(0, CHUNKS, update, 0)
    mine = pltpu.make_async_copy(cells_out.at[me], out.at[:, span(me, cells)], own_out)
    mine.start()
    drain(pred_in.at[pl.ds(0, n - 1)], data_send.at[0])
    drain(noise_in.at[pl.ds(0, n - 1)], data_send.at[1])

    @pl.when(core == 0)
    def _():
        drain(cells_in.at[pl.ds(0, n - 1)], in_send)
        drain(cells_in.at[pl.ds(0, n - 2), :, pl.ds(0, RELAYED * width)], relayed_send)

    @pl.when(core == 1)
    def _():
        if RELAYED < CHUNKS:
            drain(cells_in.at[pl.ds(0, n - 1), :, pl.ds(0, (CHUNKS - RELAYED) * width)], in_send)
        drain(members, relay_send)
        drain(cells_in.at[0, :, pl.ds(0, RELAYED * width)], beside_send)
        drain(weights, weight_send)
        drain(total.at[pl.ds(0, half * lines)], rs_send.at[0])
        drain(total.at[pl.ds(0, (half - 1) * lines)], rs_send.at[1])
        drain(total.at[pl.ds(0, half * lines)], ag_send.at[0])
        drain(total.at[pl.ds(0, (half - 1) * lines)], ag_send.at[1])

    drain(cells_out.at[pl.ds(0, n - 1)], out_send)
    drain(cells_out.at[pl.ds(0, n - 1)], out_sem)
    mine.wait()


def solution(mesh):
    n = mesh.shape[ROWS]

    def on_device(members, predicted, noise, observed, spread):
        local = members.shape[0]
        count, nz = n * local, n // 2
        cells, data = members.shape[1] // n, predicted.shape[1] // n
        half, blocks = nz // 2, count // BLOCK
        packed = (blocks * (blocks + 1) // 2 + blocks * blocks) * BLOCK
        lines = packed // nz
        anywhere = pl.BlockSpec(memory_space=pltpu.HBM)
        on_chip = pl.BlockSpec(memory_space=pltpu.VMEM)
        dma = pltpu.SemaphoreType.DMA
        return pl.pallas_call(
            functools.partial(kernel, n),
            name="smoother",
            out_shape=pltpu.VMEM(members.shape, members.dtype),
            in_specs=[anywhere, anywhere, anywhere, on_chip, on_chip],
            out_specs=on_chip,
            scratch_shapes=[
                pltpu.VMEM((n, local, data), BF16),
                pltpu.VMEM((n, local, data), BF16),
                pltpu.VMEM((n, local, cells), BF16),
                pltpu.VMEM((n, local, cells), BF16),
                pltpu.VMEM(members.shape, BF16),
                pltpu.VMEM((count, data), BF16),
                pltpu.VMEM((count, data), BF16),
                pltpu.VMEM((packed, BLOCK), F32),
                pltpu.VMEM((packed, BLOCK), F32),
                pltpu.VMEM((half, lines, BLOCK), F32),
                pltpu.VMEM((half, lines, BLOCK), F32),
                pltpu.VMEM((half, lines, BLOCK), F32),
                pltpu.VMEM((half, lines, BLOCK), F32),
                pltpu.VMEM((packed, BLOCK), F32),
                pltpu.VMEM((count, 2 * count), F32),
                pltpu.VMEM((BLOCK, BLOCK), F32),
                pltpu.VMEM((count, count), BF16),
                pltpu.VMEM((count, cells // CHUNKS), BF16),
                dma((3,)), dma((2,)), dma((2,)), dma, dma((CHUNKS,)), dma, dma, dma, dma,
                dma((2,)), dma((2, half)), dma((2, half)), dma((2,)), dma((2, half)), dma((2, half)),
                dma, dma, dma, dma, dma, dma, dma,
                pltpu.SemaphoreType.REGULAR((half - 1,)), pltpu.SemaphoreType.REGULAR((half - 1,)),
            ],
            compiler_params=pltpu.CompilerParams(
                collective_id=0, has_side_effects=True, vmem_limit_bytes=59 * 2**20
            ),
        )(members, predicted, noise, observed.reshape(1, data), spread.reshape(1, data))

    placed = (P(ROWS, "fields"), P(ROWS, "fields"), P(ROWS, "fields"), P(("fields", ROWS)), P(("fields", ROWS)))
    return jax.shard_map(
        on_device, mesh=mesh, in_specs=placed, out_specs=P(ROWS, "fields"), check_vma=False
    )
```
